16 devices in a mesh: dp: 1, tp: 16 (over x, y, z, core).
Axes of the slice: x: 2, y: 2, z: 2, core: 2. Of those that a mesh axis runs over, the one named last changes fastest.
Arguments:
- x: bfloat16 [64, 4608], P('dp')
- k_cache: bfloat16 [64, 4096, 16, 128], P('dp', None, 'tp')
- v_cache: bfloat16 [64, 4096, 16, 128], P('dp', None, 'tp')
- gain_a: bfloat16 [4608], replicated
- wq: bfloat16 [4608, 4096], P(None, 'tp')
- wo: bfloat16 [4096, 4608], P('tp')
- gain_m: bfloat16 [4608], replicated
- w_gate: bfloat16 [4608, 36864], P(None, 'tp')
- w_up: bfloat16 [4608, 36864], P(None, 'tp')
- w_down: bfloat16 [36864, 4608], P('tp')
Outputs:
- output: bfloat16 [64, 4608], P('dp')
All inputs are finite; a program needn't handle non-finite values.
Results may differ from the reference program's by a relative error of at most 0.017.
Values are sent between devices in bfloat16 or wider.
A program may use at most 2 GiB of HBM per device.

```python
import jax
import jax.numpy as jnp
from jax import lax

BATCH = 64
CACHE = 4096
D = 4608
HEADS = 32
KV_HEADS = 16
HEAD = 128
FF = 36864
THETA = 10000


def setup_inputs(seed: int = 0, part: int = 0) -> dict:
    kx, kc, kw, kn, kq, ko, km, kg, ku, kd = jax.random.split(jax.random.key(seed), 10)
    kx, kc, kw = (jax.random.fold_in(k, part) for k in (kx, kc, kw))

    def weights(key, rows, columns):
        return jax.random.normal(key, (rows, columns), jnp.float32) * rows**-0.5

    drawn = {
        "x": jax.random.normal(kx, (BATCH, D), jnp.float32),
        "k_cache": 2 * jax.random.normal(kc, (BATCH, CACHE, KV_HEADS, HEAD), jnp.float32),
        "v_cache": 4 * jax.random.normal(kw, (BATCH, CACHE, KV_HEADS, HEAD), jnp.float32),
        "gain_a": 1 + 0.1 * jax.random.normal(kn, (D,), jnp.float32),
        "wq": 2 * weights(kq, D, HEADS * HEAD),
        "wo": weights(ko, HEADS * HEAD, D),
        "gain_m": 1 + 0.1 * jax.random.normal(km, (D,), jnp.float32),
        "w_gate": weights(kg, D, FF),
        "w_up": weights(ku, D, FF),
        "w_down": 2 * weights(kd, FF, D),
    }
    return {k: v.astype(jnp.bfloat16) for k, v in drawn.items()}


def normed(x, gain):
    wide = x.astype(jnp.float32)
    scale = lax.rsqrt(jnp.mean(wide * wide, -1, keepdims=True) + 1e-6)
    return (wide * scale * gain.astype(jnp.float32)).astype(jnp.bfloat16)


def turned(t, place, theta):
    half = t.shape[-1] // 2
    angle = place.astype(jnp.float32)[:, None] * theta ** (-jnp.arange(half, dtype=jnp.float32) / half)
    cos, sin = jnp.cos(angle)[:, None], jnp.sin(angle)[:, None]
    a, b = t[..., :half].astype(jnp.float32), t[..., half:].astype(jnp.float32)
    return jnp.concatenate([a * cos - b * sin, b * cos + a * sin], -1).astype(jnp.bfloat16)


def matmul(a, w):
    return jnp.dot(a, w, preferred_element_type=jnp.float32).astype(jnp.bfloat16)


def einsum(form, a, b):
    return jnp.einsum(form, a.astype(jnp.float32), b.astype(jnp.float32))


def seen_by(a, wq, k_cache, v_cache, head, theta):
    batch, cache, kv_heads = k_cache.shape[:3]
    place = jnp.full((batch,), cache - 1)
    q = turned(matmul(a, wq).reshape(batch, -1, head), place, theta).reshape(batch, kv_heads, -1, head)
    scores = einsum("bgsd,bugd->bgsu", q, k_cache) * head**-0.5
    weights = jax.nn.softmax(scores, -1).astype(jnp.bfloat16)
    return einsum("bgsu,bugd->bgsd", weights, v_cache).astype(jnp.bfloat16).reshape(batch, -1)


def hidden_of(b, w_gate, w_up):
    gate = jnp.dot(b, w_gate, preferred_element_type=jnp.float32)
    up = jnp.dot(b, w_up, preferred_element_type=jnp.float32)
    return (jax.nn.silu(gate) * up).astype(jnp.bfloat16)


def reference(x, k_cache, v_cache, gain_a, wq, wo, gain_m, w_gate, w_up, w_down):
    seen = seen_by(normed(x, gain_a), wq, k_cache, v_cache, HEAD, THETA)
    h = (x.astype(jnp.float32) + jnp.dot(seen, wo, preferred_element_type=jnp.float32)).astype(jnp.bfloat16)
    hidden = hidden_of(normed(h, gain_m), w_gate, w_up)
    return (h.astype(jnp.float32) + jnp.dot(hidden, w_down, preferred_element_type=jnp.float32)).astype(jnp.bfloat16)
```

```python
import functools

import jax
import jax.numpy as jnp
import numpy as np
from jax import lax
from jax.experimental import pallas as pl
from jax.experimental.pallas import tpu as pltpu
from jax.sharding import PartitionSpec as P

BATCH = 64
CACHE = 4096
D = 4608
HEAD = 128
FFD = 2304
THETA = 10000
N = 16
SLOTS = 24
AHEAD = 4
GROUPS = BATCH // 4
ROWS = 16
UNIT = D // 4
CHUNKS = 3
WIDE = D // CHUNKS
PART = WIDE // 4
KEYS = 512

MESH = pl.DeviceIdType.MESH


def rms(wide, squares, gain):
    return wide * lax.rsqrt(squares / D + 1e-6) * gain


def dot_t(a, b):
    return lax.dot_general(a, b, (((1,), (1,)), ((), ())), preferred_element_type=jnp.float32)


def dot(a, b):
    return jnp.dot(a, b, preferred_element_type=jnp.float32)


def layer(x_ref, ga_ref, gm_ref, cos_ref, sin_ref, k_ref, v_ref, wq_ref, wo_ref, wg_ref, wu_ref, wd_ref, y_ref,
          ring, wo_buf, a_buf, q_buf, o_buf, term, got, h_buf, hid, term2, got2, y_buf,
          ring_sem, wo_sem, y_sem, s1, r1, s2, r2, s3, r3, s4, r4):
    me = lax.axis_index("tp")
    my_row = pl.multiple_of((me // 4) * ROWS, ROWS)
    my_col = me % 4

    def send(src, dst, ss, rs, peer):
        return pltpu.make_async_remote_copy(src_ref=src, dst_ref=dst, send_sem=ss, recv_sem=rs,
                                            device_id={"tp": peer}, device_id_type=MESH)

    def peers(body):
        def one(p, carry):
            body(lax.rem(me + p, N))
            return carry
        lax.fori_loop(1, N, one, 0)

    def cache(g, c):
        slot = lax.rem(g, SLOTS // 4) * 4 + c
        src = k_ref if c < 2 else v_ref
        return [pltpu.make_async_copy(src.at[4 * g + 2 * (c % 2) + i], ring.at[slot, i, pl.ds(0, CACHE)], ring_sem.at[slot, i])
                for i in range(2)]

    def stripe(j):
        slot = lax.rem(j + 16, SLOTS)
        cols = pl.ds(pl.multiple_of(j * 128, 128), 128)
        return [pltpu.make_async_copy(w.at[:, cols], ring.at[slot, i], ring_sem.at[slot, i]) for i, w in enumerate((wg_ref, wu_ref))]

    def down(k):
        slot = k + 10
        return [pltpu.make_async_copy(wd_ref.at[:, pl.ds(pl.multiple_of(k * 512 + c * 128, 128), 128)],
                                      ring.at[slot, c % 2, pl.ds(c // 2 * FFD, FFD)], ring_sem.at[slot, c]) for c in range(4)]

    def start(copies):
        for copy in copies:
            copy.start()

    def wait(copies):
        for copy in copies:
            copy.wait()

    wq_slot = SLOTS - 4
    wq_copies = [pltpu.make_async_copy(wq_ref.at[:, pl.ds(128 * i, 128)], ring.at[wq_slot, i], ring_sem.at[wq_slot, i]) for i in range(2)]
    wo_copy = pltpu.make_async_copy(wo_ref, wo_buf, wo_sem)
    start(wq_copies)
    for g in range(2):
        for c in range(4):
            start(cache(g, c))
    barrier = pltpu.get_barrier_semaphore()
    peers(lambda peer: pl.semaphore_signal(barrier, inc=1, device_id={"tp": peer}, device_id_type=MESH))
    wo_copy.start()
    for g in range(2, AHEAD):
        for c in range(4):
            start(cache(g, c))

    for i in range(4):
        rows = slice(16 * i, 16 * i + 16)
        wide = x_ref[rows, :].astype(jnp.float32)
        a_buf[rows, :] = rms(wide, jnp.sum(wide * wide, -1, keepdims=True), ga_ref[...].astype(jnp.float32)).astype(jnp.bfloat16)
    wait(wq_copies)
    q = dot(a_buf[...], jnp.concatenate([ring[wq_slot, 0], ring[wq_slot, 1]], 1)).astype(jnp.bfloat16).astype(jnp.float32)
    q_rows = jnp.zeros((2 * BATCH, HEAD), jnp.float32)
    row = lax.broadcasted_iota(jnp.int32, (2 * BATCH, BATCH), 0)
    col = lax.broadcasted_iota(jnp.int32, (2 * BATCH, BATCH), 1)
    for head in range(2):
        t = q[:, head * HEAD:(head + 1) * HEAD]
        t = (t * cos_ref[...] + pltpu.roll(t, HEAD // 2, 1) * sin_ref[...]).astype(jnp.bfloat16)
        q_rows += dot(jnp.where(row == 2 * col + head, 1.0, 0.0).astype(jnp.bfloat16), t)
    odd = lax.broadcasted_iota(jnp.int32, (2 * BATCH, HEAD), 0) // 2 % 2
    q_buf[:, :HEAD] = jnp.where(odd == 0, q_rows, 0.0)
    q_buf[:, HEAD:] = jnp.where(odd == 1, q_rows, 0.0)

    def attend(g, carry):
        ahead = g + AHEAD

        @pl.when(ahead < GROUPS)
        def _():
            for c in range(4):
                start(cache(ahead, c))

        @pl.when(ahead >= GROUPS)
        def _():
            for c in range(4):
                start(stripe((ahead - GROUPS) * 4 + c))

        slot = lax.rem(g, SLOTS // 4) * 4
        rows = pl.ds(pl.multiple_of(g * 8, 8), 8)
        first = lax.broadcasted_iota(jnp.int32, (8, 2 * HEAD), 0) < 4
        q8 = q_buf[rows, :]
        qs = [jnp.where(first, q8, 0.0).astype(jnp.bfloat16), jnp.where(first, 0.0, q8).astype(jnp.bfloat16)]
        wait(cache(g, 0))
        wait(cache(g, 1))
        scores = []
        for b in range(CACHE // KEYS):
            keys = slice(b * KEYS, (b + 1) * KEYS)
            s = sum(dot_t(qs[c], jnp.concatenate([ring[slot + c, 0, keys], ring[slot + c, 1, keys]], 1)) for c in range(2))
            scores.append(s * HEAD**-0.5)
        s = jnp.concatenate(scores, 1)
        e = jnp.exp(s - jnp.max(s, -1, keepdims=True))
        w = (e / jnp.sum(e, -1, keepdims=True)).astype(jnp.bfloat16)
        wait(cache(g, 2))
        wait(cache(g, 3))
        outs = [dot(w, jnp.concatenate([ring[slot + 2 + c, 0, :CACHE], ring[slot + 2 + c, 1, :CACHE]], 1)) for c in range(2)]
        out = jnp.where(first, outs[0], outs[1])
        odd8 = lax.broadcasted_iota(jnp.int32, (8, HEAD), 0) // 2 % 2
        o_buf[rows, :] = jnp.where(odd8 == 0, out[:, :HEAD], out[:, HEAD:])
        return carry

    lax.fori_loop(0, GROUPS, attend, 0)
    for j in range(4 * AHEAD, 18):
        start(stripe(j))
    for k in range(6):
        start(down(k))

    seen = [o_buf[pl.ds(head, BATCH, 2), :].astype(jnp.bfloat16) for head in range(2)]
    seen = jnp.concatenate(seen, 1)
    wo_copy.wait()
    for c in range(4):
        t = dot(seen, wo_buf[:, c * UNIT:(c + 1) * UNIT]).astype(jnp.bfloat16)
        for i in range(4):
            term[4 * i + c] = t[16 * i:16 * i + 16]
    pl.semaphore_wait(barrier, N - 1)
    peers(lambda peer: send(term.at[peer], got.at[me], s1.at[peer], r1.at[me], peer).start())
    got[me] = term[me]
    peers(lambda peer: send(term.at[peer], got.at[peer], s1.at[peer], r1.at[peer], peer).wait_recv())
    total = got[0].astype(jnp.float32)
    for p in range(1, N):
        total += got[p].astype(jnp.float32)
    block = (pl.ds(my_row, ROWS), pl.ds(pl.multiple_of(my_col * UNIT, 128), UNIT))
    h_buf[block] = (x_ref[block].astype(jnp.float32) + total).astype(jnp.bfloat16)
    peers(lambda peer: send(h_buf.at[block], h_buf.at[block], s2.at[peer], r2.at[me], peer).start())
    peers(lambda peer: send(h_buf.at[block], h_buf.at[block], s2.at[peer], r2.at[peer], peer).wait_recv())

    for i in range(4):
        rows = slice(16 * i, 16 * i + 16)
        wide = h_buf[rows, :].astype(jnp.float32)
        a_buf[rows, :] = rms(wide, jnp.sum(wide * wide, -1, keepdims=True), gm_ref[...].astype(jnp.float32)).astype(jnp.bfloat16)

    def gate_up(j, carry):
        slot = lax.rem(j + 16, SLOTS)
        wait(stripe(j))
        t = dot(a_buf[...], jnp.concatenate([ring[slot, 0], ring[slot, 1]], 1))
        gate, up = t[:, :128], t[:, 128:]
        hid[:, pl.ds(pl.multiple_of(j * 128, 128), 128)] = (gate * jax.nn.sigmoid(gate) * up).astype(jnp.bfloat16)
        return carry

    lax.fori_loop(0, 3, gate_up, 0)
    for k in range(6, 9):
        start(down(k))
    lax.fori_loop(3, 18, gate_up, 0)

    def out_block(k):
        return pl.ds(my_row, ROWS), pl.ds(pl.multiple_of(k * WIDE + my_col * PART, 128), PART)

    def product(k):
        for t in range(3):
            slot = 3 * k + t + 10
            wait(down(3 * k + t))
            for half in range(2):
                r = slice(half * FFD, (half + 1) * FFD)
                out = dot(hid[...], jnp.concatenate([ring[slot, 0, r], ring[slot, 1, r]], 1)).astype(jnp.bfloat16)
                for s in range(2):
                    piece = 4 * t + 2 * half + s
                    c, off = piece // 3, piece % 3 * 128
                    for i in range(4):
                        term2[k, 4 * i + c, :, off:off + 128] = out[16 * i:16 * i + 16, s * 128:s * 128 + 128]
        peers(lambda peer: send(term2.at[k, peer], got2.at[k, me], s3.at[k, peer], r3.at[k, me], peer).start())

    def finish(k):
        got2[k, me] = term2[k, me]
        peers(lambda peer: send(term2.at[k, peer], got2.at[k, peer], s3.at[k, peer], r3.at[k, peer], peer).wait_recv())
        total = got2[k, 0].astype(jnp.float32)
        for p in range(1, N):
            total += got2[k, p].astype(jnp.float32)
        block = out_block(k)
        y_buf[block] = (h_buf[block].astype(jnp.float32) + total).astype(jnp.bfloat16)
        peers(lambda peer: send(y_buf.at[block], y_buf.at[block], s4.at[k, peer], r4.at[k, me], peer).start())

    def chunk(k, carry):
        product(k)

        @pl.when(k > 0)
        def _():
            finish(k - 1)
        return carry

    lax.fori_loop(0, CHUNKS, chunk, 0)
    finish(CHUNKS - 1)

    def settle(k, carry):
        block = out_block(k)
        peers(lambda peer: send(y_buf.at[block], y_buf.at[block], s4.at[k, peer], r4.at[k, peer], peer).wait_recv())
        return carry

    lax.fori_loop(0, CHUNKS, settle, 0)
    out_copy = pltpu.make_async_copy(y_buf, y_ref, y_sem)
    out_copy.start()

    def sent(peer):
        send(term.at[peer], got.at[me], s1.at[peer], r1.at[me], peer).wait_send()
        block = (pl.ds(my_row, ROWS), pl.ds(pl.multiple_of(my_col * UNIT, 128), UNIT))
        send(h_buf.at[block], h_buf.at[block], s2.at[peer], r2.at[me], peer).wait_send()
        for k in range(CHUNKS):
            send(term2.at[k, peer], got2.at[k, me], s3.at[k, peer], r3.at[k, me], peer).wait_send()
            block = out_block(k)
            send(y_buf.at[block], y_buf.at[block], s4.at[k, peer], r4.at[k, me], peer).wait_send()

    peers(sent)
    out_copy.wait()


def solution(mesh):
    angle = (np.float32(CACHE - 1) * np.float32(THETA) ** (-np.arange(HEAD // 2, dtype=np.float32) / np.float32(HEAD // 2))).astype(np.float32)
    cos, sin = np.cos(angle).astype(np.float32), np.sin(angle).astype(np.float32)
    turn_cos = np.concatenate([cos, cos])[None]
    turn_sin = np.concatenate([-sin, sin])[None]

    def step(x, k_cache, v_cache, gain_a, wq, wo, gain_m, w_gate, w_up, w_down):
        vmem, hbm = pl.BlockSpec(memory_space=pltpu.VMEM), pl.BlockSpec(memory_space=pl.ANY)
        bf, dma = jnp.bfloat16, pltpu.SemaphoreType.DMA
        return pl.pallas_call(
            layer,
            out_shape=jax.ShapeDtypeStruct((BATCH, D), bf),
            in_specs=[vmem] * 5 + [hbm] * 7,
            out_specs=hbm,
            scratch_shapes=[
                pltpu.VMEM((SLOTS, 2, D, 128), bf),
                pltpu.VMEM((2 * HEAD, D), bf),
                pltpu.VMEM((BATCH, D), bf),
                pltpu.VMEM((2 * BATCH, 2 * HEAD), jnp.float32),
                pltpu.VMEM((2 * BATCH, HEAD), jnp.float32),
                pltpu.VMEM((N, ROWS, UNIT), bf),
                pltpu.VMEM((N, ROWS, UNIT), bf),
                pltpu.VMEM((BATCH, D), bf),
                pltpu.VMEM((BATCH, FFD), bf),
                pltpu.VMEM((CHUNKS, N, ROWS, PART), bf),
                pltpu.VMEM((CHUNKS, N, ROWS, PART), bf),
                pltpu.VMEM((BATCH, D), bf),
                dma((SLOTS, 4)), dma(()), dma(()),
                dma((N,)), dma((N,)), dma((N,)), dma((N,)),
                dma((CHUNKS, N)), dma((CHUNKS, N)), dma((CHUNKS, N)), dma((CHUNKS, N)),
            ],
            compiler_params=pltpu.CompilerParams(collective_id=0, has_side_effects=True, vmem_limit_bytes=67_043_328),
        )(x, gain_a[None], gain_m[None], jnp.asarray(turn_cos), jnp.asarray(turn_sin),
          k_cache.reshape(BATCH, CACHE, HEAD), v_cache.reshape(BATCH, CACHE, HEAD), wq, wo, w_gate, w_up, w_down)

    states, cache, columns, rows_of = P("dp", None), P("dp", None, "tp", None), P(None, "tp"), P("tp", None)
    return jax.shard_map(
        step,
        mesh=mesh,
        in_specs=(states, cache, cache, P(None), columns, rows_of, P(None), columns, columns, rows_of),
        out_specs=states,
        check_vma=False,
    )
```
